256 devices in a mesh: dp: 8 (over y, core), expert: 32 (over x, z).
Axes of the slice: x: 4, y: 4, z: 8, core: 2. Of those that a mesh axis runs over, the one named last changes fastest.
Arguments:
- tokens: bfloat16 [32768, 2048], P(('dp', 'expert')), may hold values from -6 to 6
- out_grad: bfloat16 [32768, 2048], P(('dp', 'expert')), may hold values from -3 to 3
- expert_ids: int32 [32768, 8], P(('dp', 'expert')), may hold values from 0 to 63, all different within a row; in each aligned block of 128 rows (0 to 127, 128 to 255, ...) at most 17 rows name the same one
- gate_probs: bfloat16 [32768, 8], P(('dp', 'expert')), may hold values from 0.019897461 to 0.3984375
- gate_up_weight: bfloat16 [64, 2048, 768], P('expert'), may hold values from -0.125 to 0.125
- down_weight: bfloat16 [64, 384, 2048], P('expert'), may hold values from -0.3125 to 0.3125
Outputs:
- grad_tokens: bfloat16 [32768, 2048], P(('dp', 'expert'))
- grad_probs: bfloat16 [32768, 8], P(('dp', 'expert'))
- grad_weights: bfloat16 [2048, 64, 1152], P('dp', 'expert')
The draws below stay inside these ranges and needn't reach their ends.
Inputs may be any that keep to these rules, and one draw needn't show every extreme that they name: `expert_ids`: each row names 8 distinct experts; in each aligned block of 128 rows no expert is named by more than 17 rows.
All inputs are finite; a program needn't handle non-finite values.
Results may differ from the reference program's by a relative error of at most 0.013.
Values may be sent and summed in bfloat16 or wider, within the bound.
A program may use at most 128 MiB of HBM per device.

```python
import math
import jax
import jax.numpy as jnp
import numpy as np
from jax import lax

D = 2048
FF = 384
TOP = 8
TOK_DEV = 128
EXPERTS = 64
MOST = 17
TOKENS = 32768
N_DP = 8
N_EXPERT = 32


def block_scale(stream_key, dims, shards, smallest, high):
    loudness, own = 1.0, jax.random.fold_in(stream_key, 6)
    for dim, blocks in shards:
        draws = jnp.exp(jax.random.uniform(jax.random.fold_in(own, dim), (blocks,), jnp.float32, smallest / len(shards), high / len(shards)))
        loudness = loudness * jnp.repeat(draws, dims[dim] // blocks).reshape([-1 if axis == dim else 1 for axis in range(len(dims))])
    return loudness


def shared_out(own_key, own, number, rows, number_of, top, most, skew):
    order = jax.random.permutation(own_key, number_of)
    heavy_load, common = portions_of(number_of, rows * top, most, skew, True), portions_of(number_of, rows * top, most, skew, False)
    places = jnp.arange(number_of)

    def named(lengths, offset_by):
        used = int((lengths > 0).sum())
        fixed = max(1, used // 4)
        moved = fixed + (places - fixed + offset_by * (used - fixed)) % max(1, number_of - fixed)
        return jnp.zeros((number_of,), jnp.int32).at[order[jnp.where(places < fixed, places, moved)]].set(jnp.asarray(lengths, jnp.int32))

    lengths = jnp.where(number % 4 == 0, named(heavy_load, number // 4), named(common, number - number // 4 - 1))
    mixed = jax.random.permutation(jax.random.fold_in(own, 3), number_of)
    giver, sink = mixed[0:number_of // 2 * 2:2], mixed[1:number_of // 2 * 2:2]
    room = jnp.minimum(lengths[giver] - 1, most - lengths[sink]) // 2
    room = jnp.where((giver == order[0]) | (sink == order[0]) | (lengths[sink] == 0), 0, jnp.maximum(room, 0))
    moved = jax.random.randint(jax.random.fold_in(own, 4), (number_of // 2,), 0, 1 << 20) % (room + 1)
    lengths = lengths.at[giver].add(-moved).at[sink].add(moved)
    items = jnp.searchsorted(jnp.cumsum(lengths), jnp.arange(rows * top), side="right").astype(jnp.int32)
    grid = items.reshape(top, rows).T
    grid = grid[jax.random.permutation(jax.random.fold_in(own, 1), rows)]
    offset_by = jax.random.randint(jax.random.fold_in(own, 2), (rows, 1), 0, top)
    return jnp.take_along_axis(grid, (jnp.arange(top)[None, :] + offset_by) % top, axis=1)


def portions_of(number_of, total, bound, skew, full):
    loads = [(1 << 20) // math.isqrt(rank ** skew) + 1 for rank in range(1, number_of + 1)]
    largest = bound if full else min(bound, max(-(-total // number_of), total * loads[0] // sum(loads)))
    least = 1 if total - largest >= number_of - 1 else 0
    holding, rest = [largest] + [least] * (number_of - 1), total - largest - least * (number_of - 1)
    while rest > 0:
        free = [i for i in range(1, number_of) if holding[i] < largest] or [i for i in range(1, number_of) if holding[i] < bound]
        mass, left = sum([loads[i] for i in free]), rest
        for i in free:
            more = min(bound - holding[i], max(1, left * loads[i] // mass), rest)
            holding[i] = holding[i] + more
            rest = rest - more
    return np.array(holding)


def centred(key, dims, spread, reach, split=(), kind=jnp.bfloat16):
    array = jax.random.normal(key, dims, jnp.float32) * spread
    if len(split) > 0:
        array = block_scale(key, dims, split, -0.22, 0.18) * array
    return jnp.clip(array, min=-reach, max=reach).astype(kind)


def setup_inputs(seed: int = 0) -> dict:
    streams_of = jax.random.split(jax.random.key(seed), 7)
    tokens = centred(streams_of[0], (TOKENS, D), 1.0, 6.0, ((0, 256),))
    out_grad = centred(streams_of[1], (TOKENS, D), 0.5, 3.0, ((0, 256),))
    expert_ids_keys = jax.random.split(jax.random.fold_in(streams_of[2], 1), TOKENS // TOK_DEV)
    expert_ids_turns = jax.random.permutation(jax.random.fold_in(streams_of[2], 3), TOKENS // TOK_DEV)
    expert_ids = jax.vmap(lambda own, number: shared_out(jax.random.fold_in(streams_of[2], 2), own, number, TOK_DEV, EXPERTS, TOP, MOST, 2))(expert_ids_keys, expert_ids_turns).reshape((TOKENS, TOP))
    gate_probs = jnp.clip(jnp.exp(math.log(0.3984375) - 2.9969585 * jax.random.uniform(streams_of[3], (TOKENS, TOP), jnp.float32) ** block_scale(streams_of[3], (TOKENS, TOP), ((0, 256),), -0.2, 0.2)), 0.019897461, 0.3984375).astype(jnp.bfloat16)
    gate_up_weight = centred(streams_of[4], (EXPERTS, D, 2 * FF), D ** -0.5, 0.125, ((0, 32),))
    down_weight = centred(streams_of[5], (EXPERTS, FF, D), FF ** -0.5, 0.3125, ((0, 32),))
    return dict(tokens=tokens, out_grad=out_grad, expert_ids=expert_ids, gate_probs=gate_probs, gate_up_weight=gate_up_weight, down_weight=down_weight)


def rounded(value):
    return lax.optimization_barrier(value.astype(jnp.bfloat16)).astype(jnp.float32)


def silu_parts(gate_pre):
    logistic = jax.nn.sigmoid(gate_pre)
    return gate_pre * logistic, logistic * (1.0 + gate_pre * (1.0 - logistic))


def reference(tokens, out_grad, expert_ids, gate_probs, gate_up_weight, down_weight):
    token_count = tokens.shape[0]
    blocks = token_count // TOK_DEV
    pair_count = token_count * TOP
    block_ids = expert_ids.reshape(blocks, TOK_DEV * TOP)
    onehot = (block_ids[:, :, None] == jnp.arange(EXPERTS, dtype=jnp.int32)[None, None, :]).astype(jnp.int32)
    ranking = jnp.sum((jnp.cumsum(onehot, axis=1) - onehot) * onehot, axis=2)
    block_index = jnp.arange(blocks, dtype=jnp.int32)[:, None]
    placement = (block_ids * blocks + block_index) * MOST + ranking
    slot_table = jnp.full((EXPERTS * blocks * MOST,), pair_count, jnp.int32)
    slot_table = slot_table.at[placement.reshape(-1)].set(jnp.arange(pair_count, dtype=jnp.int32))
    slot_table = slot_table.reshape(EXPERTS, blocks * MOST)
    flat_probs = gate_probs.reshape(-1)

    def one_expert(carry, inputs):
        grad_rows, grad_gate = carry
        slot_index, weight_in, weight_out = inputs
        filled = slot_index < pair_count
        clipped = jnp.minimum(slot_index, pair_count - 1)
        owner_token = clipped // TOP
        inputs_rows = jnp.where(filled[:, None], tokens[owner_token], 0).astype(jnp.float32)
        cotangent = jnp.where(filled[:, None], out_grad[owner_token], 0).astype(jnp.float32)
        weights_rows = jnp.where(filled, flat_probs[clipped], 0).astype(jnp.float32)
        weight_in32 = weight_in.astype(jnp.float32)
        weight_out32 = weight_out.astype(jnp.float32)
        pre_acts = jnp.dot(inputs_rows, weight_in32, preferred_element_type=jnp.float32)
        gate_pre = pre_acts[:, :FF]
        up_pre = pre_acts[:, FF:]
        active, slope_terms = silu_parts(gate_pre)
        hidden = rounded(active * up_pre)
        expert_out = jnp.dot(hidden, weight_out32, preferred_element_type=jnp.float32)
        gate_grad = jnp.sum(cotangent * expert_out, axis=1).astype(jnp.bfloat16)
        scaled = rounded(weights_rows[:, None] * cotangent)
        grad_hidden = jnp.dot(scaled, weight_out32.T, preferred_element_type=jnp.float32)
        grad_pre = rounded(jnp.concatenate([grad_hidden * up_pre * slope_terms, grad_hidden * active], axis=1))
        row_grad = rounded(jnp.dot(grad_pre, weight_in32.T, preferred_element_type=jnp.float32))
        grad_rows = grad_rows.at[jnp.where(filled, owner_token, token_count)].add(row_grad, mode="drop")
        grad_gate = grad_gate.at[slot_index].set(gate_grad, mode="drop")
        inputs_dp = inputs_rows.reshape(N_DP, N_EXPERT * MOST, D)
        pre_dp = grad_pre.reshape(N_DP, N_EXPERT * MOST, 2 * FF)
        scaled_dp = scaled.reshape(N_DP, N_EXPERT * MOST, D)
        hidden_dp = hidden.reshape(N_DP, N_EXPERT * MOST, FF)
        part_in = jnp.einsum("prd,prf->pdf", inputs_dp, pre_dp)
        part_out = jnp.einsum("prd,prf->pdf", scaled_dp, hidden_dp)
        partial_value = rounded(jnp.concatenate([part_in, part_out], axis=2))
        summed = jnp.sum(partial_value, axis=0).astype(jnp.bfloat16)
        return (grad_rows, grad_gate), summed

    start_rows = jnp.zeros((token_count, D), jnp.float32)
    start_gate = jnp.zeros((pair_count,), jnp.bfloat16)
    (grad_rows, grad_gate), stacked = lax.scan(one_expert, (start_rows, start_gate), (slot_table, gate_up_weight, down_weight))
    grad_weights = jnp.transpose(stacked, (1, 0, 2))
    return grad_rows.astype(jnp.bfloat16), grad_gate.reshape(token_count, TOP), grad_weights
```

```python
import functools
import jax
import jax.numpy as jnp
from jax import lax
from jax.experimental import pallas as pl
from jax.experimental.pallas import tpu as pltpu
from jax.sharding import PartitionSpec as P

X = 4
CAP = 17
W = 256
H = 128
MESH = pl.DeviceIdType.MESH
F32 = jnp.float32
BF16 = jnp.bfloat16


def dot(a, b, ca=1, cb=0):
    return lax.dot_general(a, b, (((ca,), (cb,)), ((), ())), preferred_element_type=F32)


def ring(v, n):
    return lax.rem(v + n, n)


def at_expert(index):
    return {"expert": index}


def greet(mx, mz, zs):
    barrier = pltpu.get_barrier_semaphore()
    for d in range(1, zs):
        pl.semaphore_signal(
            barrier, inc=1, device_id=at_expert(mx * zs + ring(mz + d, zs)), device_id_type=MESH
        )
    for d in range(1, X):
        pl.semaphore_signal(
            barrier, inc=1, device_id=at_expert(ring(mx + d, X) * zs + mz), device_id_type=MESH
        )
    pl.semaphore_wait(barrier, zs - 1 + X - 1)


def remote(src, dst, send_sem, recv_sem, device):
    return pltpu.make_async_remote_copy(
        src_ref=src,
        dst_ref=dst,
        send_sem=send_sem,
        recv_sem=recv_sem,
        device_id=at_expert(device),
        device_id_type=MESH,
    )


def rows_of(block, n):
    return pl.ds(pl.multiple_of(block * n, n), n)


def dispatch_kernel(
    zs, half, tok, cot, meta, wgu, wd, gp_o, gg_o, mt_o, wp_o,
    zbuf, metab, xmeta, pick, xs, xr, rl, accp, accu, wguv, wdv, hs, wst,
    own_sem, w_sem, wst_sem, z_send, z_recv, x_send, x_recv, r_recv, m_send, m_recv, q_send, q_recv,
):
    t = tok.shape[0]
    ff = wd.shape[1]
    chunks = 2 * half
    rpe = zs * CAP
    rows = 2 * rpe
    expert = lax.axis_index("expert")
    mx, mz = expert // zs, lax.rem(expert, zs)
    zn, zp = mx * zs + ring(mz + 1, zs), mx * zs + ring(mz - 1, zs)
    xn, xp = ring(mx + 1, X) * zs + mz, ring(mx - 1, X) * zs + mz
    far = zs // 2

    w_copies = [
        pltpu.make_async_copy(wgu, wguv, w_sem.at[0]),
        pltpu.make_async_copy(wd, wdv, w_sem.at[1]),
        pltpu.make_async_copy(
            meta.at[mz], metab.at[:, :, rows_of(mz, t)], w_sem.at[2]
        ),
    ]
    own = rows_of(mz, t)

    def own_copy(src, c, lanes):
        return pltpu.make_async_copy(
            src.at[:, pl.ds(pl.multiple_of(lanes * W, W), W)], zbuf.at[c, own], own_sem.at[c]
        )

    @pl.loop(0, half)
    def _(c):
        own_copy(tok, c, c).start()
        own_copy(cot, c + half, c).start()

    for copy in w_copies:
        copy.start()
    greet(mx, mz, zs)

    def meta_copy(d):
        peer = ring(mz + d, zs)
        return remote(
            meta.at[peer], metab.at[:, :, rows_of(mz, t)], m_send.at[d], m_recv.at[d],
            mx * zs + peer,
        )

    for d in range(1, zs):
        meta_copy(d).start()

    def z_copy(c, way, h):
        block = ring(mz - h, zs) if way == 0 else ring(mz + h, zs)
        ref = zbuf.at[c, rows_of(block, t)]
        if h == far - 1:
            ref = zbuf.at[c, rows_of(block, t), pl.ds(way * H, H)]
        return remote(
            ref, ref, z_send.at[c, way, h], z_recv.at[c, way, h], zn if way == 0 else zp
        )

    def z_wait(c, way, h):
        block = ring(mz - h - 1, zs) if way == 0 else ring(mz + h + 1, zs)
        ref = zbuf.at[c, rows_of(block, t)]
        if h == far - 1:
            ref = zbuf.at[c, rows_of(block, t), pl.ds(way * H, H)]
        return remote(
            ref, ref, z_send.at[c, way, h], z_recv.at[c, way, h], zn if way == 0 else zp
        )

    def x_copies(c):
        return (
            remote(xs.at[c, 0], xr.at[c, 1], x_send.at[c, 0], x_recv.at[c, 0], xn),
            remote(xs.at[c, 2], xr.at[c, 3], x_send.at[c, 1], x_recv.at[c, 1], xp),
            remote(
                xs.at[c, 1, :, pl.ds(0, H)], rl.at[c, 0], x_send.at[c, 2], r_recv.at[c, 0], xn
            ),
            remote(
                xs.at[c, 1, :, pl.ds(H, H)], rl.at[c, 1], x_send.at[c, 3], r_recv.at[c, 1], xp
            ),
        )

    def relay_copies(c):
        return (
            remote(
                rl.at[c, 0], xr.at[c, 2, :, pl.ds(0, H)], x_send.at[c, 4], x_recv.at[c, 2], xn
            ),
            remote(
                rl.at[c, 1], xr.at[c, 2, :, pl.ds(H, H)], x_send.at[c, 5], x_recv.at[c, 3], xp
            ),
        )

    def quick_copy(d):
        peer = ring(mx + d, X)
        return remote(
            metab.at[peer], xmeta.at[d], q_send.at[d], q_recv.at[d], peer * zs + mz
        )

    accp[...] = jnp.zeros_like(accp)
    accu[...] = jnp.zeros_like(accu)

    def valid(c):
        return (c >= 0) & (c < chunks)

    @pl.loop(0, chunks + far + 3)
    def _(i):
        @pl.when(i < chunks)
        def _():
            own_copy(tok, i, 0).wait()
            z_copy(i, 0, 0).start()
            z_copy(i, 1, 0).start()

        for h in range(1, far):
            @pl.when(valid(i - h))
            def _():
                c = i - h
                for way in range(2):
                    z_wait(c, way, h - 1).wait_recv()
                    z_copy(c, way, h).start()

        @pl.when(i == far - 1)
        def _():
            w_copies[2].wait()
            for d in range(1, zs):
                meta_copy(d).wait_recv()
            for d in range(1, X):
                quick_copy(d).start()
            for d in range(X):
                peer = ring(mx + d, X)
                first = jnp.broadcast_to(metab[peer, 0:1, :], (16, zs * t))
                second = jnp.broadcast_to(metab[peer, 1:2, :], (16, zs * t))

                @pl.loop(0, rows // 16)
                def _(b):
                    ids = lax.broadcasted_iota(jnp.int32, (16, zs * t), 0) + b * 16
                    slot = ids.astype(F32)
                    hit = jnp.where(ids < rpe, first, second) == slot
                    pick[d, pl.ds(pl.multiple_of(b * 16, 16), 16), :] = jnp.where(
                        hit, 1.0, 0.0
                    ).astype(BF16)

        @pl.when(valid(i - far))
        def _():
            c = i - far
            for way in range(2):
                z_wait(c, way, far - 1).wait_recv()
            for d in (2, 1, 3, 0):
                got = dot(pick[d], zbuf[c]).astype(BF16)
                if d == 0:
                    xr[c, 0] = got
                else:
                    xs[c, d - 1] = got
            direct = x_copies(c)
            for k in (2, 3, 0, 1):
                direct[k].start()

        @pl.when(valid(i - far - 1))
        def _():
            c = i - far - 1
            into = x_copies(c)
            out = relay_copies(c)
            for way in range(2):
                into[2 + way].wait_recv()
                out[way].start()

        @pl.when(i == far + 1)
        def _():
            w_copies[0].wait()
            w_copies[1].wait()

        def arrived(c):
            direct, passed = x_copies(c), relay_copies(c)
            direct[0].wait_recv()
            direct[1].wait_recv()
            passed[0].wait_recv()
            passed[1].wait_recv()

        @pl.when((i >= far + 2) & (i < far + 2 + half))
        def _():
            c = i - far - 2
            arrived(c)

            @pl.loop(0, X)
            def _(s):
                for e in range(2):
                    lo = e * (rpe // 16 * 16)
                    cut = e * rpe - lo
                    part = dot(
                        xr[c, s, pl.ds(lo, rows - rpe // 16 * 16)],
                        wguv[e, pl.ds(pl.multiple_of(c * W, W), W), :],
                    )
                    at = pl.ds(pl.multiple_of(s * rows + e * rpe, 8), rpe)
                    accp[at, :] += part[cut : cut + rpe]

        @pl.when((i >= far + 2 + half) & (i < far + 2 + chunks))
        def _():
            c = i - far - 2
            arrived(c)

            @pl.loop(0, X)
            def _(s):
                for e in range(2):
                    lo = e * (rpe // 16 * 16)
                    cut = e * rpe - lo
                    part = dot(
                        xr[c, s, pl.ds(lo, rows - rpe // 16 * 16)],
                        wdv[e, :, pl.ds(pl.multiple_of((c - half) * W, W), W)],
                        1,
                        1,
                    )
                    at = pl.ds(pl.multiple_of(s * rows + e * rpe, 8), rpe)
                    accu[at, :] += part[cut : cut + rpe]

    for d in range(1, X):
        quick_copy(d).wait_recv()
    xmeta[0] = metab[mx]
    mt_o[...] = metab[...]
    padded = rows - rpe // 16 * 16

    @pl.loop(0, X)
    def _(s):
        sums = []
        for e in range(2):
            at = pl.ds(pl.multiple_of(s * rows + e * rpe, 8), rpe)
            slot = xmeta[s, e : e + 1, :]
            gate_row = xmeta[s, 2 + e : 3 + e, :]
            ids = (lax.broadcasted_iota(jnp.int32, (rpe, zs * t), 0) + e * rpe).astype(F32)
            gate = jnp.sum(jnp.where(slot == ids, gate_row, 0.0), axis=1, keepdims=True)
            gate_pre = accp[at, 0:ff]
            up_pre = accp[at, ff : 2 * ff]
            logistic = jax.nn.sigmoid(gate_pre)
            active = gate_pre * logistic
            slope = logistic * (1.0 + gate_pre * (1.0 - logistic))
            hidden = (active * up_pre).astype(BF16).astype(F32)
            u = accu[at, :]
            sums.append(jnp.sum(hidden * u, axis=1, keepdims=True))
            gh = gate * u
            full = jnp.concatenate([gh * up_pre * slope, gh * active], axis=1)
            scaled_hidden = gate * hidden
            gap = padded - rpe
            if e == 0:
                full = jnp.concatenate([full, jnp.zeros((gap, 2 * ff), F32)], axis=0)
                scaled_hidden = jnp.concatenate([scaled_hidden, jnp.zeros((gap, ff), F32)], axis=0)
            else:
                full = jnp.concatenate([jnp.zeros((gap, 2 * ff), F32), full], axis=0)
                scaled_hidden = jnp.concatenate([jnp.zeros((gap, ff), F32), scaled_hidden], axis=0)
            gp_o[e, s] = full.astype(BF16)
            hs[e, s] = scaled_hidden.astype(BF16)
        wide = gg_o.shape[2]
        column = jnp.concatenate(sums + [jnp.zeros((wide - rows, 1), F32)], axis=0)
        a = lax.broadcasted_iota(jnp.int32, (wide, wide), 0)
        b = lax.broadcasted_iota(jnp.int32, (wide, wide), 1)
        diagonal = jnp.where(a == b, column, 0.0).astype(BF16)
        row = lax.broadcasted_iota(jnp.int32, (16, wide), 0)
        lane = lax.broadcasted_iota(jnp.int32, (16, wide), 1)
        mine = ((row == 0) & (lane < rpe)) | ((row == 1) & (lane >= rpe) & (lane < rows))
        gg_o[s] = dot(jnp.where(mine, 1.0, 0.0).astype(BF16), diagonal).astype(BF16)

    def out_copy(c, slot):
        return pltpu.make_async_copy(wst.at[slot], wp_o.at[c], wst_sem.at[slot])

    @pl.loop(0, half)
    def _(c):
        slot = lax.rem(c, 2)

        @pl.when(c >= 2)
        def _():
            out_copy(c, slot).wait()

        for e in range(2):
            lo = e * (rpe // 16 * 16)
            first = dot(xr[c, 0, pl.ds(lo, padded)], gp_o[e, 0], 0, 0)
            second = dot(xr[c + half, 0, pl.ds(lo, padded)], hs[e, 0], 0, 0)
            for s in range(1, X):
                first += dot(xr[c, s, pl.ds(lo, padded)], gp_o[e, s], 0, 0)
                second += dot(xr[c + half, s, pl.ds(lo, padded)], hs[e, s], 0, 0)
            wst[slot, e, :, 0 : 2 * ff] = first.astype(BF16)
            wst[slot, e, :, 2 * ff : 3 * ff] = second.astype(BF16)
        out_copy(c, slot).start()

    for c in range(half - 2, half):
        out_copy(c, c % 2).wait()
    for d in range(1, zs):
        meta_copy(d).wait_send()
    for d in range(1, X):
        quick_copy(d).wait_send()

    @pl.loop(0, chunks)
    def _(c):
        for h in range(far):
            for way in range(2):
                z_copy(c, way, h).wait_send()
        for copy in x_copies(c) + relay_copies(c):
            copy.wait_send()


def combine_kernel(
    zs, half, gp, gg, mt, wgu, out, dp_o,
    wguv, pick, rs, rr, rl, part, zo, zi, ggr, dps, dpr,
    w_sem, z_send, z_recv, x_send, x_recv, r_recv, g_send, g_recv, d_send, d_recv,
):
    t = out.shape[0]
    rpe = zs * CAP
    rows = 2 * rpe
    wide = gg.shape[2]
    padded = rows - rpe // 16 * 16
    expert = lax.axis_index("expert")
    mx, mz = expert // zs, lax.rem(expert, zs)
    zn, zp = mx * zs + ring(mz + 1, zs), mx * zs + ring(mz - 1, zs)
    xn, xp = ring(mx + 1, X) * zs + mz, ring(mx - 1, X) * zs + mz
    far = zs // 2

    w_copy = pltpu.make_async_copy(wgu, wguv, w_sem.at[0])
    w_copy.start()
    greet(mx, mz, zs)

    def gate_copy(s):
        return remote(
            gg.at[s], ggr.at[s], g_send.at[s], g_recv.at[s], ring(mx - s, X) * zs + mz
        )

    for s in range(1, X):
        gate_copy(s).start()

    for d in range(X):
        peer = ring(mx + d, X)
        first = jnp.broadcast_to(mt[peer, 0:1, :], (16, zs * t))
        second = jnp.broadcast_to(mt[peer, 1:2, :], (16, zs * t))

        @pl.loop(0, wide // 16)
        def _(b):
            ids = lax.broadcasted_iota(jnp.int32, (16, zs * t), 0) + b * 16
            slot = ids.astype(F32)
            hit = jnp.where(ids < rpe, first, second) == slot
            pick[d, pl.ds(pl.multiple_of(b * 16, 16), 16), :] = jnp.where(hit, 1.0, 0.0).astype(
                BF16
            )

    w_copy.wait()

    def x_copies(c):
        return (
            remote(rs.at[c, 0], rr.at[c, 1], x_send.at[c, 0], x_recv.at[c, 0], xp),
            remote(rs.at[c, 2], rr.at[c, 3], x_send.at[c, 1], x_recv.at[c, 1], xn),
            remote(
                rs.at[c, 1, :, pl.ds(0, H)], rl.at[c, 0], x_send.at[c, 2], r_recv.at[c, 0], xp
            ),
            remote(
                rs.at[c, 1, :, pl.ds(H, H)], rl.at[c, 1], x_send.at[c, 3], r_recv.at[c, 1], xn
            ),
        )

    def relay_copies(c):
        return (
            remote(
                rl.at[c, 0], rr.at[c, 2, :, pl.ds(0, H)], x_send.at[c, 4], x_recv.at[c, 2], xp
            ),
            remote(
                rl.at[c, 1], rr.at[c, 2, :, pl.ds(H, H)], x_send.at[c, 5], x_recv.at[c, 3], xn
            ),
        )

    def z_copy(c, way, h):
        src, dst = zo.at[c, way, h], zi.at[c, way, h]
        if h == 0:
            src, dst = src.at[:, pl.ds(way * H, H)], dst.at[:, pl.ds(way * H, H)]
        return remote(
            src, dst, z_send.at[c, way, h], z_recv.at[c, way, h], zn if way == 0 else zp
        )

    def piece(c, block):
        return part[c, rows_of(block, t), :]

    def valid(c):
        return (c >= 0) & (c < half)

    def probs_copy(d):
        peer = ring(mz + d, zs)
        return remote(
            dps.at[:, :, rows_of(peer, t)], dpr.at[mz], d_send.at[d], d_recv.at[d],
            mx * zs + peer,
        )

    def probs_wait(d):
        peer = ring(mz - d, zs)
        return remote(
            dps.at[:, :, rows_of(peer, t)], dpr.at[peer], d_send.at[d], d_recv.at[d],
            mx * zs + peer,
        )

    @pl.loop(0, half + far + 2)
    def _(i):
        @pl.when(i < half)
        def _():
            lanes = rows_of(i, W)
            for s in (2, 1, 3, 0):
                both = []
                for e in range(2):
                    res = dot(gp[e, s], wguv[e, lanes, :], 1, 1)
                    cut = e * (padded - rpe)
                    both.append(res[cut : cut + rpe])
                got = jnp.concatenate(both, axis=0).astype(BF16)
                if s == 0:
                    rr[i, 0] = got
                else:
                    rs[i, s - 1] = got
            direct = x_copies(i)
            for k in (2, 3, 0, 1):
                direct[k].start()

        @pl.when(i == 1)
        def _():
            for s in range(1, X):
                gate_copy(s).wait_recv()
            ggr[0] = gg[0]
            for d in range(X):
                dps[d] = dot(ggr[d], pick[d])
            for d in range(1, zs):
                probs_copy(d).start()

        @pl.when(valid(i - 1))
        def _():
            c = i - 1
            into, onward = x_copies(c), relay_copies(c)
            for way in range(2):
                into[2 + way].wait_recv()
                onward[way].start()

        @pl.when(valid(i - 2))
        def _():
            c = i - 2
            direct, passed = x_copies(c), relay_copies(c)
            direct[0].wait_recv()
            direct[1].wait_recv()
            passed[0].wait_recv()
            passed[1].wait_recv()
            total = dot(pick[0, 0:rows, :], rr[c, 0], 0, 0)
            for d in range(1, X):
                total += dot(pick[d, 0:rows, :], rr[c, d], 0, 0)
            part[c] = total
            for way in range(2):
                zo[c, way, 0] = piece(c, ring(mz + far, zs)).astype(BF16)
                z_copy(c, way, 0).start()

        for h in range(1, far):
            @pl.when(valid(i - 2 - h))
            def _():
                c = i - 2 - h
                for way in range(2):
                    z_copy(c, way, h - 1).wait_recv()
                    block = ring(mz + far - h, zs) if way == 0 else ring(mz - far + h, zs)
                    mine = piece(c, block)
                    if h == 1:
                        side = pl.ds(way * H, H)
                        other = pl.ds(H - way * H, H)
                        lo, hi = way * H, H - way * H
                        zo[c, way, h, :, side] = (
                            mine[:, lo : lo + H] + zi[c, way, 0, :, side].astype(F32)
                        ).astype(BF16)
                        zo[c, way, h, :, other] = mine[:, hi : hi + H].astype(BF16)
                    else:
                        zo[c, way, h] = (mine + zi[c, way, h - 1].astype(F32)).astype(BF16)
                    z_copy(c, way, h).start()

        @pl.when(valid(i - 2 - far))
        def _():
            c = i - 2 - far
            for way in range(2):
                z_copy(c, way, far - 1).wait_recv()
            total = piece(c, mz)
            total += zi[c, 0, far - 1].astype(F32) + zi[c, 1, far - 1].astype(F32)
            out[:, rows_of(c, W)] = total.astype(BF16)

    dpr[mz] = dps[:, :, rows_of(mz, t)]
    for d in range(1, zs):
        probs_wait(d).wait_recv()
    dp_o[...] = dpr[...]
    for d in range(1, zs):
        probs_copy(d).wait_send()
    for s in range(1, X):
        gate_copy(s).wait_send()

    @pl.loop(0, half)
    def _(c):
        for h in range(far):
            for way in range(2):
                z_copy(c, way, h).wait_send()
        for copy in x_copies(c) + relay_copies(c):
            copy.wait_send()


def on_device(tokens, out_grad, expert_ids, gate_probs, gate_up_weight, down_weight):
    t, width = tokens.shape
    top = expert_ids.shape[1]
    ff = down_weight.shape[1]
    zs = lax.axis_size("expert") // X
    experts = 2 * X * zs
    half = width // W
    chunks = 2 * half
    far = zs // 2
    rpe = zs * CAP
    rows = 2 * rpe
    padded = rows - rpe // 16 * 16
    wide = -(-rows // 128) * 128
    mz = lax.rem(lax.axis_index("expert"), zs)

    named = expert_ids.T[:, None, :] == jnp.arange(experts, dtype=jnp.int32)[None, :, None]
    hit = jnp.any(named, axis=0)
    gates = jnp.sum(jnp.where(named, gate_probs.T[:, None, :].astype(F32), 0.0), axis=0)
    before = (
        jnp.arange(t, dtype=jnp.int32)[:, None] < jnp.arange(t, dtype=jnp.int32)[None, :]
    )
    rank = jnp.dot(hit.astype(BF16), before.astype(BF16), preferred_element_type=F32)
    base = mz * CAP + (jnp.arange(experts, dtype=jnp.int32) % 2) * rpe
    slots = jnp.where(hit, rank + base.astype(F32)[:, None], -1.0)
    both = jnp.stack([slots, gates]).reshape(2, X, zs, 2, t)
    meta = jnp.pad(
        both.transpose(2, 1, 0, 3, 4).reshape(zs, X, 4, t), ((0, 0), (0, 0), (0, 4), (0, 0))
    )

    hbm = pl.BlockSpec(memory_space=pltpu.MemorySpace.HBM)
    vmem = pl.BlockSpec(memory_space=pltpu.MemorySpace.VMEM)
    dma = pltpu.SemaphoreType.DMA
    gp, gg, mt, weight_part = pl.pallas_call(
        functools.partial(dispatch_kernel, zs, half),
        out_shape=(
            jax.ShapeDtypeStruct((2, X, padded, 2 * ff), BF16),
            jax.ShapeDtypeStruct((X, 16, wide), BF16),
            jax.ShapeDtypeStruct((X, 8, zs * t), F32),
            jax.ShapeDtypeStruct((half, 2, W, 3 * ff), BF16),
        ),
        in_specs=[hbm] * 5,
        out_specs=(vmem, vmem, vmem, hbm),
        scratch_shapes=[
            pltpu.VMEM((chunks, zs * t, W), BF16),
            pltpu.VMEM((X, 8, zs * t), F32),
            pltpu.VMEM((X, 8, zs * t), F32),
            pltpu.VMEM((X, rows, zs * t), BF16),
            pltpu.VMEM((chunks, X - 1, rows, W), BF16),
            pltpu.VMEM((chunks, X, rows, W), BF16),
            pltpu.VMEM((chunks, 2, rows, H), BF16),
            pltpu.VMEM((X * rows, 2 * ff), F32),
            pltpu.VMEM((X * rows, ff), F32),
            pltpu.VMEM((2, width, 2 * ff), BF16),
            pltpu.VMEM((2, ff, width), BF16),
            pltpu.VMEM((2, X, padded, ff), BF16),
            pltpu.VMEM((2, 2, W, 3 * ff), BF16),
            dma((chunks,)),
            dma((3,)),
            dma((2,)),
            dma((chunks, 2, far)),
            dma((chunks, 2, far)),
            dma((chunks, 6)),
            dma((chunks, 4)),
            dma((chunks, 2)),
            dma((zs,)),
            dma((zs,)),
            dma((X,)),
            dma((X,)),
        ],
        compiler_params=pltpu.CompilerParams(
            collective_id=0, has_side_effects=True, vmem_limit_bytes=61 * 1024 * 1024
        ),
        cost_estimate=pl.CostEstimate(
            flops=20_000_000_000, bytes_accessed=30_000_000, transcendentals=0
        ),
        name="dispatch",
    )(tokens, out_grad, meta, gate_up_weight, down_weight)

    summed = lax.psum_scatter(weight_part, "dp", scatter_dimension=0, tiled=True)

    grad_tokens, probs = pl.pallas_call(
        functools.partial(combine_kernel, zs, half),
        out_shape=(
            jax.ShapeDtypeStruct((t, width), BF16),
            jax.ShapeDtypeStruct((zs, X, 16, t), F32),
        ),
        in_specs=[vmem, vmem, vmem, hbm],
        out_specs=(vmem, vmem),
        scratch_shapes=[
            pltpu.VMEM((2, width, 2 * ff), BF16),
            pltpu.VMEM((X, wide, zs * t), BF16),
            pltpu.VMEM((half, X - 1, rows, W), BF16),
            pltpu.VMEM((half, X, rows, W), BF16),
            pltpu.VMEM((half, 2, rows, H), BF16),
            pltpu.VMEM((half, zs * t, W), F32),
            pltpu.VMEM((half, 2, far, t, W), BF16),
            pltpu.VMEM((half, 2, far, t, W), BF16),
            pltpu.VMEM((X, 16, wide), BF16),
            pltpu.VMEM((X, 16, zs * t), F32),
            pltpu.VMEM((zs, X, 16, t), F32),
            dma((1,)),
            dma((half, 2, far)),
            dma((half, 2, far)),
            dma((half, 6)),
            dma((half, 4)),
            dma((half, 2)),
            dma((X,)),
            dma((X,)),
            dma((zs,)),
            dma((zs,)),
        ],
        compiler_params=pltpu.CompilerParams(
            collective_id=1, has_side_effects=True, vmem_limit_bytes=61 * 1024 * 1024
        ),
        cost_estimate=pl.CostEstimate(
            flops=60_000_000_000, bytes_accessed=100_000_000, transcendentals=0
        ),
        name="combine",
    )(gp, gg, mt, gate_up_weight)

    mx = lax.axis_index("expert") // zs
    order = (jnp.arange(X, dtype=jnp.int32) - mx) % X
    by_expert = probs[:, :, 0:2, :][:, order]
    by_expert = by_expert.transpose(1, 0, 2, 3).reshape(experts, t)
    grad_probs = jnp.sum(jnp.where(named, by_expert[None], 0.0), axis=1).T.astype(BF16)
    grad_weights = summed.transpose(0, 2, 1, 3).reshape(-1, 2, 3 * ff)
    return (grad_tokens, grad_probs, grad_weights)


def solution(mesh):
    split = P(("dp", "expert"), None)
    return jax.shard_map(
        on_device,
        mesh=mesh,
        in_specs=(split, split, split, split, P("expert", None, None), P("expert", None, None)),
        out_specs=(split, split, P("dp", "expert", None)),
        check_vma=False,
    )
```
